32 devices in a mesh: replica: 2 (over x), data2: 4 (over z), data: 4 (over y, core).
Axes of the slice: x: 2, y: 2, z: 4, core: 2. Of those that a mesh axis runs over, the one named last changes fastest.
Arguments:
- q_hidden: bfloat16 [256, 32, 2048], P(('replica', 'data2', 'data')), parts along dimension 0
- d_hidden: bfloat16 [256, 768, 2048], P(('replica', 'data2', 'data')), parts along dimension 0
- w_proj: bfloat16 [2048, 128], replicated
- q_mask: int32 [256, 32], P(('replica', 'data2', 'data')), parts along dimension 0
- d_mask: int32 [256, 768], P(('replica', 'data2', 'data')), parts along dimension 0
- temperature: float32 [], replicated
Outputs:
- output 1: float32 [256], P(('replica', 'data2', 'data')), parts along dimension 0
- output 2: float32 [2], P('replica'), parts along dimension 0
There are 2 independent parts. The reference program is written for one: setup_inputs(seed, part) draws one part's arguments, and reference() takes and returns one part's arrays. A program takes and returns all parts, laid end to end along the dimension named above; an argument that names none is the same for every part.
All inputs are finite; a program needn't handle non-finite values.
Results may differ from the reference program's by a relative error of at most 0.00218619.
Values are sent between devices in bfloat16 or wider.
A program may use at most 1 GiB of HBM per device.

```python
import math
import jax
import jax.numpy as jnp
from jax import lax

BATCH = 128
QLEN = 32
DLEN = 768
HIDDEN = 2048
PROJ = 128

NORM_EPS = 1e-6
TAU_SCALE = QLEN / (8.0 * math.log(BATCH))


def setup_inputs(seed: int = 0, part: int = 0) -> dict:
    base_key = jax.random.key(seed)
    rand_keys = jax.random.split(jax.random.fold_in(base_key, part), 7)
    shared = jax.random.normal(rand_keys[0], (HIDDEN,), jnp.float32)
    doc_len = jax.random.randint(rand_keys[1], (BATCH,), DLEN // 2, DLEN + 1)
    qry_len = jax.random.randint(rand_keys[2], (BATCH,), QLEN // 2, QLEN + 1)
    doc_mask = (jnp.arange(DLEN)[None, :] < doc_len[:, None]).astype(jnp.int32)
    qry_mask = (jnp.arange(QLEN)[None, :] < qry_len[:, None]).astype(jnp.int32)
    doc_noise = jax.random.normal(rand_keys[3], (BATCH, DLEN, HIDDEN), jnp.float32)
    src_pos = jax.random.randint(rand_keys[4], (BATCH, QLEN), 0, doc_len[:, None])
    src_idx = jnp.broadcast_to(src_pos[:, :, None], (BATCH, QLEN, HIDDEN))
    copied = jnp.take_along_axis(doc_noise, src_idx, axis=1)
    share_w = jax.random.uniform(rand_keys[5], (BATCH, 1, 1), jnp.float32, 0.15, 0.4)
    fresh = jax.random.normal(rand_keys[6], (BATCH, QLEN, HIDDEN), jnp.float32)
    half_amp = math.sqrt(0.5)
    d_keep = doc_mask[:, :, None] > 0
    d_hidden = jnp.where(d_keep, half_amp, 2.0) * shared + jnp.where(d_keep, half_amp, 0.3) * doc_noise
    q_keep = qry_mask[:, :, None] > 0
    q_mix = jnp.sqrt(share_w) * copied + jnp.sqrt(1.0 - share_w) * fresh
    q_body = jnp.where(q_keep, q_mix, copied)
    q_hidden = jnp.where(q_keep, 1.0, 2.5) * (half_amp * shared + half_amp * q_body)
    w_proj = jax.random.normal(jax.random.fold_in(base_key, 1000), (HIDDEN, PROJ), jnp.float32) * HIDDEN ** -0.5
    temperature = jax.random.uniform(jax.random.fold_in(base_key, 2000), (), jnp.float32, 0.6, 1.4) * TAU_SCALE
    return {
        'q_hidden': q_hidden.astype(jnp.bfloat16),
        'd_hidden': d_hidden.astype(jnp.bfloat16),
        'w_proj': w_proj.astype(jnp.bfloat16),
        'q_mask': qry_mask,
        'd_mask': doc_mask,
        'temperature': temperature.astype(jnp.float32),
    }


def project(hidden, w_proj):
    flat_rows = hidden.reshape(-1, hidden.shape[-1])
    proj_f32 = jnp.dot(flat_rows, w_proj, preferred_element_type=jnp.float32)
    row_norm = jnp.sqrt(jnp.sum(proj_f32 * proj_f32, axis=-1, keepdims=True) + NORM_EPS)
    unit_rows = (proj_f32 / row_norm).astype(jnp.bfloat16)
    return unit_rows.reshape(hidden.shape[:-1] + (w_proj.shape[1],))


def reference(q_hidden, d_hidden, w_proj, q_mask, d_mask, temperature):
    q_tok = project(q_hidden, w_proj).astype(jnp.float32)
    d_tok = project(d_hidden, w_proj).astype(jnp.float32)
    d_valid = d_mask > 0
    q_weight = q_mask.astype(jnp.float32)

    def score_row(row_in):
        q_row, weight_row = row_in
        sim_vals = jnp.einsum('td,psd->tps', q_row, d_tok)
        best_sim = jnp.max(jnp.where(d_valid[None], sim_vals, -jnp.inf), axis=-1)
        return jnp.sum(weight_row[:, None] * best_sim, axis=0)

    scores = lax.map(score_row, (q_tok, q_weight))
    logits = scores / temperature
    row_max = jnp.max(logits, axis=1, keepdims=True)
    log_norm = row_max[:, 0] + jnp.log(jnp.sum(jnp.exp(logits - row_max), axis=1))
    loss_rows = log_norm - jnp.diagonal(logits)
    return loss_rows, jnp.mean(loss_rows).reshape(1)
```

```python
import jax
import jax.numpy as jnp
from jax import lax
from jax.experimental import pallas as pl
from jax.experimental.pallas import tpu as pltpu
from jax.sharding import PartitionSpec as P

NORM_EPS = 1e-6
ROW_AXES = ('replica', 'data2', 'data')
MESH = pl.DeviceIdType.MESH
F32, BF16 = jnp.float32, jnp.bfloat16
MASKED = -1e30

DOCS, DLEN, QLEN, HID, PROJ = 8, 768, 32, 2048, 128
ROWS = DOCS * DLEN
CHUNK = 512
NCHUNK = ROWS // CHUNK
TILE = 256
GROUP = 2
SGROUP = 2
QROWS = DOCS * QLEN
NBLK, NCHIP = 16, 8


def kernel(q_hbm, d_hbm, w_hbm, qm_hbm, dm_hbm, t_hbm, loss_ref, mean_ref,
           x, qh, wv, ext, qall, qf, bias, rs, sall, qm, dm, tv,
           dsem, isem, bsend, brecv, fsend, frecv, ssend, srecv):
    z, d = lax.axis_index('data2'), lax.axis_index('data')
    y, c = d // 2, d % 2
    me = z * 4 + d

    def peer(k):
        ky, k0, k1 = k % 2, (k // 2) % 2, k // 4
        pz = (z % 2 + k0) % 2 + 2 * ((z // 2 + k1) % 2)
        return pz, ((y + ky) % 2) * 2 + c

    def chip_of(k):
        pz, pd = peer(k)
        return pz * 2 + pd // 2

    def send_block(k):
        pz, pd = peer(k)
        return pltpu.make_async_remote_copy(
            src_ref=qall.at[me], dst_ref=qall.at[me], send_sem=bsend.at[k], recv_sem=brecv.at[k],
            device_id={'data2': pz, 'data': pd}, device_id_type=MESH)

    def recv_block(k):
        pz, pd = peer(k)
        blk = pz * 4 + pd
        return pltpu.make_async_remote_copy(
            src_ref=qall.at[blk], dst_ref=qall.at[blk], send_sem=bsend.at[k], recv_sem=brecv.at[k],
            device_id={'data2': pz, 'data': pd}, device_id_type=MESH)

    def forward(k):
        blk = chip_of(k) * 2 + c
        return pltpu.make_async_remote_copy(
            src_ref=qall.at[blk], dst_ref=qall.at[blk], send_sem=fsend.at[k], recv_sem=frecv.at[k],
            device_id={'data2': z, 'data': y * 2 + 1 - c}, device_id_type=MESH)

    def recv_forward(k):
        blk = chip_of(k) * 2 + 1 - c
        return pltpu.make_async_remote_copy(
            src_ref=qall.at[blk], dst_ref=qall.at[blk], send_sem=fsend.at[k], recv_sem=frecv.at[k],
            device_id={'data2': z, 'data': y * 2 + 1 - c}, device_id_type=MESH)

    def any_peer(k):
        pz, pd = peer(k // 2)
        return pz, (pd // 2) * 2 + (c + k % 2) % 2

    def send_scores(k):
        pz, pd = any_peer(k)
        return pltpu.make_async_remote_copy(
            src_ref=sall.at[me], dst_ref=sall.at[me], send_sem=ssend.at[k], recv_sem=srecv.at[k],
            device_id={'data2': pz, 'data': pd}, device_id_type=MESH)

    def recv_scores(k):
        pz, pd = any_peer(k)
        blk = pz * 4 + pd
        return pltpu.make_async_remote_copy(
            src_ref=sall.at[blk], dst_ref=sall.at[blk], send_sem=ssend.at[k], recv_sem=srecv.at[k],
            device_id={'data2': pz, 'data': pd}, device_id_type=MESH)

    def chunk_copy(t):
        return pltpu.make_async_copy(d_hbm.at[pl.ds(pl.multiple_of(t * CHUNK, CHUNK), CHUNK), :], x.at[t], dsem.at[t])

    copies = [pltpu.make_async_copy(a, b, isem.at[i]) for i, (a, b) in enumerate(
        ((w_hbm, wv), (q_hbm, qh), (qm_hbm, qm), (dm_hbm, dm), (t_hbm, tv)))]
    for copy in copies:
        copy.start()
    for t in range(NCHUNK):
        chunk_copy(t).start()

    barrier = pltpu.get_barrier_semaphore()
    for k in range(1, NBLK):
        pz, pd = any_peer(k)
        pl.semaphore_signal(barrier, inc=1, device_id={'data2': pz, 'data': pd}, device_id_type=MESH)

    def unit(proj):
        return proj * lax.rsqrt(jnp.sum(proj * proj, axis=1, keepdims=True) + NORM_EPS)

    def dot(a, b):
        return lax.dot_general(a, b, (((1,), (0,)), ((), ())), preferred_element_type=F32)

    for i in range(3):
        copies[i].wait()
    qf[...] = unit(dot(qh[...], wv[...]))
    rows = []
    for t in range(QLEN):
        keep = qm[:, t:t + 1] > 0
        rows.append(jnp.where(keep, qf[pl.ds(t, DOCS, stride=QLEN), :], 0.0))
    qall[me] = jnp.concatenate(rows, axis=0).astype(BF16)

    copies[3].wait()
    pad = jnp.where(dm[...] > 0, 0.0, MASKED).astype(F32)
    pad = jnp.concatenate([pad, jnp.zeros((120, DLEN), F32)], axis=0)
    for i in range(DLEN // 128):
        bias[pl.ds(i * 128, 128), :] = pad[:, i * 128:(i + 1) * 128].T
    lane = lax.broadcasted_iota(jnp.int32, (TILE, 128), 1)

    def project_chunk(t):
        chunk_copy(t).wait()
        row = pl.multiple_of(t * CHUNK, CHUNK)
        ext[pl.ds(row, CHUNK), 0:128] = unit(dot(x[t], wv[...])).astype(BF16)
        for n in range(CHUNK // TILE):
            tile = t * (CHUNK // TILE) + n
            part = bias[pl.ds(pl.multiple_of((tile % 3) * TILE, TILE), TILE), :]
            ext[pl.ds(row + n * TILE, TILE), 128:256] = jnp.where(lane == tile // 3, part, 0.0).astype(BF16)

    def project_group(i, _):
        for n in range(GROUP):
            project_chunk(i * GROUP + n)
        return 0

    project_group(0, 0)
    pl.semaphore_wait(barrier, NBLK - 1)
    forward(0).start()
    for k in range(1, NCHIP):
        send_block(k).start()
    lax.fori_loop(1, NCHUNK // GROUP - 1, project_group, 0)
    recv_block(1).wait_recv()
    forward(1).start()
    project_group(NCHUNK // GROUP - 1, 0)

    ones_ext = jnp.where(lane < DOCS, 1.0, 0.0).astype(BF16)

    def stage(p, fwd, nxt):
        chip = chip_of(p)
        blocks = [jnp.concatenate([qall[chip * 2 + q], ones_ext], axis=1) for q in (0, 1)]
        for j in range(DOCS):
            if j == DOCS // 2:
                if fwd:
                    recv_block(p + 2).wait_recv()
                    forward(p + 2).start()
                if nxt:
                    recv_forward(p + 1).wait_recv()
            for q in (0, 1):
                sim = lax.dot_general(ext[pl.ds(j * DLEN, DLEN), :], blocks[q], (((1,), (1,)), ((), ())), preferred_element_type=F32)
                best = jnp.max(sim.reshape(DLEN // 8, 8, TILE), axis=0)
                rs[q, pl.ds(chip * DOCS + j, 1), :] = jnp.max(best, axis=0, keepdims=True)

    def stages(i, _):
        for n in range(SGROUP):
            stage(i * SGROUP + n, True, True)
        return 0

    recv_forward(0).wait_recv()
    lax.fori_loop(0, (NCHIP - 2) // SGROUP, stages, 0)
    stage(NCHIP - 2, False, True)
    stage(NCHIP - 1, False, False)

    half = lax.broadcasted_iota(jnp.int32, (DOCS, 128), 1)
    vals = []
    for b in range(NBLK):
        v = rs[b % 2, pl.ds(8 * (b // 2), 8), :]
        vals.append(v[:, :128] + v[:, 128:])
    for width in (64, 32, 16, 8):
        n = len(vals) // 2
        low = (half // width) % 2 == 0
        nxt = []
        for i in range(n):
            keep = jnp.where(low, vals[i], vals[i + n])
            move = jnp.where(low, vals[i + n], vals[i])
            fold = jnp.where(low, pltpu.roll(move, 128 - width, axis=1), pltpu.roll(move, width, axis=1)) if width < 64 else pltpu.roll(move, 64, axis=1)
            nxt.append(keep + fold)
        vals = nxt
    sall[me] = vals[0]

    for k in range(1, NBLK):
        send_scores(k).start()
    copies[4].wait()
    temp = tv[0]
    for k in range(1, NBLK):
        recv_scores(k).wait_recv()
    logits = sall[...] / temp
    top = jnp.max(jnp.max(logits, axis=0), axis=0, keepdims=True)
    total = jnp.sum(jnp.sum(jnp.exp(logits - top[None]), axis=0), axis=0, keepdims=True)
    doc = lax.broadcasted_iota(jnp.int32, (NBLK, DOCS, 128), 0) * DOCS + lax.broadcasted_iota(jnp.int32, (NBLK, DOCS, 128), 1)
    own = doc == lax.broadcasted_iota(jnp.int32, (NBLK, DOCS, 128), 2)
    pos = jnp.sum(jnp.sum(jnp.where(own, logits, 0.0), axis=0), axis=0, keepdims=True)
    loss = top + jnp.log(total) - pos
    mean_ref[...] = jnp.sum(loss, axis=1, keepdims=True) / (NBLK * DOCS)
    loss_ref[...] = pltpu.roll(jnp.broadcast_to(loss, (8, 128)), lax.rem(128 - me * DOCS, 128), axis=1)[0:1, :DOCS]

    for k in range(1, NCHIP):
        send_block(k).wait_send()
    for k in range(NCHIP):
        forward(k).wait_send()
    for k in range(1, NBLK):
        send_scores(k).wait_send()


def solution(mesh):
    def device_fn(q_hidden, d_hidden, w_proj, q_mask, d_mask, temperature):
        hbm = pl.BlockSpec(memory_space=pltpu.HBM)
        vmem = pl.BlockSpec(memory_space=pltpu.VMEM)
        dma = pltpu.SemaphoreType.DMA
        loss, mean = pl.pallas_call(
            kernel,
            out_shape=(jax.ShapeDtypeStruct((1, DOCS), F32), jax.ShapeDtypeStruct((1, 1), F32)),
            in_specs=[hbm] * 6,
            out_specs=(vmem, vmem),
            scratch_shapes=[
                pltpu.VMEM((NCHUNK, CHUNK, HID), BF16),
                pltpu.VMEM((QROWS, HID), BF16),
                pltpu.VMEM((HID, PROJ), BF16),
                pltpu.VMEM((ROWS, 256), BF16),
                pltpu.VMEM((NBLK, QROWS, PROJ), BF16),
                pltpu.VMEM((QROWS, PROJ), F32),
                pltpu.VMEM((DLEN, 128), F32),
                pltpu.VMEM((2, DOCS * NCHIP, 256), F32),
                pltpu.VMEM((NBLK, DOCS, 128), F32),
                pltpu.VMEM((DOCS, QLEN), jnp.int32),
                pltpu.VMEM((DOCS, DLEN), jnp.int32),
                pltpu.SMEM((1,), F32),
                dma((NCHUNK,)), dma((5,)), dma((NCHIP,)), dma((NCHIP,)), dma((NCHIP,)), dma((NCHIP,)), dma((NBLK,)), dma((NBLK,)),
            ],
            compiler_params=pltpu.CompilerParams(collective_id=0, has_side_effects=True, vmem_limit_bytes=60 * 2**20),
            name='late_interaction',
        )(q_hidden.reshape(QROWS, HID), d_hidden.reshape(ROWS, HID), w_proj, q_mask, d_mask, temperature.reshape(1))
        return loss.reshape(DOCS), mean.reshape(1)

    return jax.shard_map(
        device_fn,
        mesh=mesh,
        in_specs=(P(ROW_AXES), P(ROW_AXES), P(), P(ROW_AXES), P(ROW_AXES), P()),
        out_specs=(P(ROW_AXES), P('replica')),
        check_vma=False,
    )
```

```python
import jax
import jax.numpy as jnp
from jax import lax
from jax.experimental import pallas as pl
from jax.experimental.pallas import tpu as pltpu
from jax.sharding import PartitionSpec as P

NORM_EPS = 1e-6
ROW_AXES = ('replica', 'data2', 'data')
MESH = pl.DeviceIdType.MESH
F32, BF16 = jnp.float32, jnp.bfloat16
MASKED = -1e30

DOCS, DLEN, QLEN, HID, PROJ = 8, 768, 32, 2048, 128
ROWS = DOCS * DLEN
CHUNK = 512
NCHUNK = ROWS // CHUNK
AHEAD = 5
STEP = 1536
NSTEP = ROWS // STEP
SGROUP = 1
TILE = 256
QROWS = DOCS * QLEN
NBLK, NCHIP = 16, 8


def kernel(q_hbm, d_hbm, w_hbm, qm_hbm, dm_hbm, t_hbm, loss_ref, mean_ref,
           x, qh, wv, ext, qall, qf, bias, rs, sall, qm, dm, tv,
           dsem, isem, bsend, brecv, fsend, frecv, ssend, srecv):
    z, d = lax.axis_index('data2'), lax.axis_index('data')
    y, c = d // 2, d % 2
    me = z * 4 + d

    def peer(k):
        ky, k0, k1 = k % 2, (k // 2) % 2, k // 4
        pz = (z % 2 + k0) % 2 + 2 * ((z // 2 + k1) % 2)
        return pz, ((y + ky) % 2) * 2 + c

    def chip_of(k):
        pz, pd = peer(k)
        return pz * 2 + pd // 2

    def send_block(k):
        pz, pd = peer(k)
        return pltpu.make_async_remote_copy(
            src_ref=qall.at[me], dst_ref=qall.at[me], send_sem=bsend.at[k], recv_sem=brecv.at[k],
            device_id={'data2': pz, 'data': pd}, device_id_type=MESH)

    def recv_block(k):
        pz, pd = peer(k)
        blk = pz * 4 + pd
        return pltpu.make_async_remote_copy(
            src_ref=qall.at[blk], dst_ref=qall.at[blk], send_sem=bsend.at[k], recv_sem=brecv.at[k],
            device_id={'data2': pz, 'data': pd}, device_id_type=MESH)

    def forward(k):
        blk = chip_of(k) * 2 + c
        return pltpu.make_async_remote_copy(
            src_ref=qall.at[blk], dst_ref=qall.at[blk], send_sem=fsend.at[k], recv_sem=frecv.at[k],
            device_id={'data2': z, 'data': y * 2 + 1 - c}, device_id_type=MESH)

    def recv_forward(k):
        blk = chip_of(k) * 2 + 1 - c
        return pltpu.make_async_remote_copy(
            src_ref=qall.at[blk], dst_ref=qall.at[blk], send_sem=fsend.at[k], recv_sem=frecv.at[k],
            device_id={'data2': z, 'data': y * 2 + 1 - c}, device_id_type=MESH)

    def any_peer(k):
        pz, pd = peer(k // 2)
        return pz, (pd // 2) * 2 + (c + k % 2) % 2

    def send_scores(k):
        pz, pd = any_peer(k)
        return pltpu.make_async_remote_copy(
            src_ref=sall.at[me], dst_ref=sall.at[me], send_sem=ssend.at[k], recv_sem=srecv.at[k],
            device_id={'data2': pz, 'data': pd}, device_id_type=MESH)

    def recv_scores(k):
        pz, pd = any_peer(k)
        blk = pz * 4 + pd
        return pltpu.make_async_remote_copy(
            src_ref=sall.at[blk], dst_ref=sall.at[blk], send_sem=ssend.at[k], recv_sem=srecv.at[k],
            device_id={'data2': pz, 'data': pd}, device_id_type=MESH)

    def chunk_copy(t):
        return pltpu.make_async_copy(d_hbm.at[pl.ds(pl.multiple_of(t * CHUNK, CHUNK), CHUNK), :],
                                     x.at[pl.ds(pl.multiple_of(t * CHUNK, CHUNK), CHUNK), :], dsem.at[t])

    copies = [pltpu.make_async_copy(a, b, isem.at[i]) for i, (a, b) in enumerate(
        ((w_hbm, wv), (q_hbm, qh), (qm_hbm, qm), (dm_hbm, dm), (t_hbm, tv)))]
    for copy in copies:
        copy.start()
    chunk_copy(0).start()

    barrier = pltpu.get_barrier_semaphore()
    for k in range(1, NBLK):
        pz, pd = any_peer(k)
        pl.semaphore_signal(barrier, inc=1, device_id={'data2': pz, 'data': pd}, device_id_type=MESH)

    def unit(proj):
        return proj * lax.rsqrt(jnp.sum(proj * proj, axis=1, keepdims=True) + NORM_EPS)

    def dot(a, b):
        return lax.dot_general(a, b, (((1,), (0,)), ((), ())), preferred_element_type=F32)

    for i in range(3):
        copies[i].wait()
    for t in range(1, AHEAD):
        chunk_copy(t).start()
    qf[...] = unit(dot(qh[...], wv[...]))
    rows = []
    for t in range(QLEN):
        keep = qm[:, t:t + 1] > 0
        rows.append(jnp.where(keep, qf[pl.ds(t, DOCS, stride=QLEN), :], 0.0))
    qall[me] = jnp.concatenate(rows, axis=0).astype(BF16)

    copies[3].wait()
    pad = jnp.where(dm[...] > 0, 0.0, MASKED).astype(F32)
    pad = jnp.concatenate([pad, jnp.zeros((120, DLEN), F32)], axis=0)
    for i in range(DLEN // 128):
        bias[pl.ds(i * 128, 128), :] = pad[:, i * 128:(i + 1) * 128].T
    lane = lax.broadcasted_iota(jnp.int32, (TILE, 128), 1)

    ones_ext = jnp.where(lane < DOCS, 1.0, 0.0).astype(BF16)

    def query_blocks(chip):
        return [jnp.concatenate([qall[chip * 2 + q], ones_ext], axis=1) for q in (0, 1)]

    def score(blocks, chip, j):
        docs = ext[pl.ds(pl.multiple_of(j * DLEN, DLEN), DLEN), :]
        for q in (0, 1):
            sim = lax.dot_general(docs, blocks[q], (((1,), (1,)), ((), ())), preferred_element_type=F32)
            best = jnp.max(sim.reshape(DLEN // 8, 8, TILE), axis=0)
            rs[q, pl.ds(chip * DOCS + j, 1), :] = jnp.max(best, axis=0, keepdims=True)

    def project_step(t, _):
        for n in range(STEP // CHUNK):
            chunk = t * (STEP // CHUNK) + n
            chunk_copy(chunk).wait()

            @pl.when(chunk < NCHUNK - AHEAD)
            def _():
                chunk_copy(chunk + AHEAD).start()

        row = pl.multiple_of(t * STEP, STEP)
        ext[pl.ds(row, STEP), 0:128] = unit(dot(x[pl.ds(row, STEP), :], wv[...])).astype(BF16)
        for n in range(STEP // TILE):
            part = bias[pl.ds((n % 3) * TILE, TILE), :]
            ext[pl.ds(row + n * TILE, TILE), 128:256] = jnp.where(lane == t * 2 + n // 3, part, 0.0).astype(BF16)
        return 0

    pl.semaphore_wait(barrier, NBLK - 1)
    forward(0).start()
    for k in range(1, NCHIP):
        send_block(k).start()
    lax.fori_loop(0, NSTEP, project_step, 0)

    for k in range(1, SGROUP):
        recv_block(k).wait_recv()
        forward(k).start()

    def stages(i, _):
        for n in range(SGROUP):
            recv_forward(i * SGROUP + n).wait_recv()

        @pl.when(i < NCHIP // SGROUP - 1)
        def _():
            for n in range(SGROUP):
                recv_block((i + 1) * SGROUP + n).wait_recv()
                forward((i + 1) * SGROUP + n).start()

        for n in range(SGROUP):
            chip = chip_of(i * SGROUP + n)
            blocks = query_blocks(chip)
            for j in range(DOCS):
                score(blocks, chip, j)
        return 0

    lax.fori_loop(0, NCHIP // SGROUP, stages, 0)

    half = lax.broadcasted_iota(jnp.int32, (DOCS, 128), 1)
    vals = []
    for b in range(NBLK):
        v = rs[b % 2, pl.ds(8 * (b // 2), 8), :]
        vals.append(v[:, :128] + v[:, 128:])
    for width in (64, 32, 16, 8):
        n = len(vals) // 2
        low = (half // width) % 2 == 0
        nxt = []
        for i in range(n):
            keep = jnp.where(low, vals[i], vals[i + n])
            move = jnp.where(low, vals[i + n], vals[i])
            fold = jnp.where(low, pltpu.roll(move, 128 - width, axis=1), pltpu.roll(move, width, axis=1)) if width < 64 else pltpu.roll(move, 64, axis=1)
            nxt.append(keep + fold)
        vals = nxt
    sall[me] = vals[0]

    for k in range(1, NBLK):
        send_scores(k).start()
    copies[4].wait()
    temp = tv[0]
    for k in range(1, NBLK):
        recv_scores(k).wait_recv()
    logits = sall[...] / temp
    top = jnp.max(jnp.max(logits, axis=0), axis=0, keepdims=True)
    total = jnp.sum(jnp.sum(jnp.exp(logits - top[None]), axis=0), axis=0, keepdims=True)
    doc = lax.broadcasted_iota(jnp.int32, (NBLK, DOCS, 128), 0) * DOCS + lax.broadcasted_iota(jnp.int32, (NBLK, DOCS, 128), 1)
    own = doc == lax.broadcasted_iota(jnp.int32, (NBLK, DOCS, 128), 2)
    pos = jnp.sum(jnp.sum(jnp.where(own, logits, 0.0), axis=0), axis=0, keepdims=True)
    loss = top + jnp.log(total) - pos
    mean_ref[...] = jnp.sum(loss, axis=1, keepdims=True) / (NBLK * DOCS)
    loss_ref[...] = pltpu.roll(jnp.broadcast_to(loss, (8, 128)), lax.rem(128 - me * DOCS, 128), axis=1)[0:1, :DOCS]

    for k in range(1, NCHIP):
        send_block(k).wait_send()
    for k in range(NCHIP):
        forward(k).wait_send()
    for k in range(1, NBLK):
        send_scores(k).wait_send()


def solution(mesh):
    def device_fn(q_hidden, d_hidden, w_proj, q_mask, d_mask, temperature):
        hbm = pl.BlockSpec(memory_space=pltpu.HBM)
        vmem = pl.BlockSpec(memory_space=pltpu.VMEM)
        dma = pltpu.SemaphoreType.DMA
        loss, mean = pl.pallas_call(
            kernel,
            out_shape=(jax.ShapeDtypeStruct((1, DOCS), F32), jax.ShapeDtypeStruct((1, 1), F32)),
            in_specs=[hbm] * 6,
            out_specs=(vmem, vmem),
            scratch_shapes=[
                pltpu.VMEM((ROWS, HID), BF16),
                pltpu.VMEM((QROWS, HID), BF16),
                pltpu.VMEM((HID, PROJ), BF16),
                pltpu.VMEM((ROWS, 256), BF16),
                pltpu.VMEM((NBLK, QROWS, PROJ), BF16),
                pltpu.VMEM((QROWS, PROJ), F32),
                pltpu.VMEM((DLEN, 128), F32),
                pltpu.VMEM((2, DOCS * NCHIP, 256), F32),
                pltpu.VMEM((NBLK, DOCS, 128), F32),
                pltpu.VMEM((DOCS, QLEN), jnp.int32),
                pltpu.VMEM((DOCS, DLEN), jnp.int32),
                pltpu.SMEM((1,), F32),
                dma((NCHUNK,)), dma((5,)), dma((NCHIP,)), dma((NCHIP,)), dma((NCHIP,)), dma((NCHIP,)), dma((NBLK,)), dma((NBLK,)),
            ],
            compiler_params=pltpu.CompilerParams(collective_id=0, has_side_effects=True, vmem_limit_bytes=60 * 2**20),
            name='late_interaction',
        )(q_hidden.reshape(QROWS, HID), d_hidden.reshape(ROWS, HID), w_proj, q_mask, d_mask, temperature.reshape(1))
        return loss.reshape(DOCS), mean.reshape(1)

    return jax.shard_map(
        device_fn,
        mesh=mesh,
        in_specs=(P(ROW_AXES), P(ROW_AXES), P(), P(ROW_AXES), P(ROW_AXES), P()),
        out_specs=(P(ROW_AXES), P('replica')),
        check_vma=False,
    )
```

```python
import jax
import jax.numpy as jnp
from jax import lax
from jax.experimental import pallas as pl
from jax.experimental.pallas import tpu as pltpu
from jax.sharding import PartitionSpec as P

NORM_EPS = 1e-6
ROW_AXES = ('replica', 'data2', 'data')
MESH = pl.DeviceIdType.MESH
F32, BF16 = jnp.float32, jnp.bfloat16
MASKED = -1e30

DOCS, DLEN, QLEN, HID, PROJ = 8, 768, 32, 2048, 128
ROWS = DOCS * DLEN
CHUNK = 512
NCHUNK = ROWS // CHUNK
AHEAD = 5
STEP = 1536
NSTEP = ROWS // STEP
SGROUP = 2
TILE = 256
QROWS = DOCS * QLEN
NBLK, NCHIP = 16, 8


def kernel(q_hbm, d_hbm, w_hbm, qm_hbm, dm_hbm, out_ref,
           x, qh, wv, ext, qall, qf, bias, rs, sall, qm, dm,
           dsem, isem, bsend, brecv, fsend, frecv, ssend, srecv):
    z, d = lax.axis_index('data2'), lax.axis_index('data')
    y, c = d // 2, d % 2
    me = z * 4 + d

    def peer(k):
        ky, k0, k1 = k % 2, (k // 2) % 2, k // 4
        pz = (z % 2 + k0) % 2 + 2 * ((z // 2 + k1) % 2)
        return pz, ((y + ky) % 2) * 2 + c

    def chip_of(k):
        pz, pd = peer(k)
        return pz * 2 + pd // 2

    def send_block(k):
        pz, pd = peer(k)
        return pltpu.make_async_remote_copy(
            src_ref=qall.at[me], dst_ref=qall.at[me], send_sem=bsend.at[k], recv_sem=brecv.at[k],
            device_id={'data2': pz, 'data': pd}, device_id_type=MESH)

    def recv_block(k):
        pz, pd = peer(k)
        blk = pz * 4 + pd
        return pltpu.make_async_remote_copy(
            src_ref=qall.at[blk], dst_ref=qall.at[blk], send_sem=bsend.at[k], recv_sem=brecv.at[k],
            device_id={'data2': pz, 'data': pd}, device_id_type=MESH)

    def forward(k):
        blk = chip_of(k) * 2 + c
        return pltpu.make_async_remote_copy(
            src_ref=qall.at[blk], dst_ref=qall.at[blk], send_sem=fsend.at[k], recv_sem=frecv.at[k],
            device_id={'data2': z, 'data': y * 2 + 1 - c}, device_id_type=MESH)

    def recv_forward(k):
        blk = chip_of(k) * 2 + 1 - c
        return pltpu.make_async_remote_copy(
            src_ref=qall.at[blk], dst_ref=qall.at[blk], send_sem=fsend.at[k], recv_sem=frecv.at[k],
            device_id={'data2': z, 'data': y * 2 + 1 - c}, device_id_type=MESH)

    def any_peer(k):
        pz, pd = peer(k // 2)
        return pz, (pd // 2) * 2 + (c + k % 2) % 2

    def send_scores(k):
        pz, pd = any_peer(k)
        return pltpu.make_async_remote_copy(
            src_ref=sall.at[me], dst_ref=sall.at[me], send_sem=ssend.at[k], recv_sem=srecv.at[k],
            device_id={'data2': pz, 'data': pd}, device_id_type=MESH)

    def recv_scores(k):
        pz, pd = any_peer(k)
        blk = pz * 4 + pd
        return pltpu.make_async_remote_copy(
            src_ref=sall.at[blk], dst_ref=sall.at[blk], send_sem=ssend.at[k], recv_sem=srecv.at[k],
            device_id={'data2': pz, 'data': pd}, device_id_type=MESH)

    def chunk_copy(t):
        return pltpu.make_async_copy(d_hbm.at[pl.ds(pl.multiple_of(t * CHUNK, CHUNK), CHUNK), :],
                                     x.at[pl.ds(pl.multiple_of(t * CHUNK, CHUNK), CHUNK), :], dsem.at[t])

    copies = [pltpu.make_async_copy(a, b, isem.at[i]) for i, (a, b) in enumerate(
        ((w_hbm, wv), (q_hbm, qh), (qm_hbm, qm), (dm_hbm, dm)))]
    for copy in copies:
        copy.start()
    chunk_copy(0).start()

    barrier = pltpu.get_barrier_semaphore()
    for k in range(1, NBLK):
        pz, pd = any_peer(k)
        pl.semaphore_signal(barrier, inc=1, device_id={'data2': pz, 'data': pd}, device_id_type=MESH)

    def unit(proj):
        return proj * lax.rsqrt(jnp.sum(proj * proj, axis=1, keepdims=True) + NORM_EPS)

    def dot(a, b):
        return lax.dot_general(a, b, (((1,), (0,)), ((), ())), preferred_element_type=F32)

    for i in range(3):
        copies[i].wait()
    for t in range(1, AHEAD):
        chunk_copy(t).start()
    qf[...] = unit(dot(qh[...], wv[...]))
    rows = []
    for t in range(QLEN):
        keep = qm[:, t:t + 1] > 0
        rows.append(jnp.where(keep, qf[pl.ds(t, DOCS, stride=QLEN), :], 0.0))
    qall[me] = jnp.concatenate(rows, axis=0).astype(BF16)

    copies[3].wait()
    pad = jnp.where(dm[...] > 0, 0.0, MASKED).astype(F32)
    pad = jnp.concatenate([pad, jnp.zeros((120, DLEN), F32)], axis=0)
    for i in range(DLEN // 128):
        bias[pl.ds(i * 128, 128), :] = pad[:, i * 128:(i + 1) * 128].T
    lane = lax.broadcasted_iota(jnp.int32, (TILE, 128), 1)

    ones_ext = jnp.where(lane < DOCS, 1.0, 0.0).astype(BF16)

    def query_blocks(chip):
        return [jnp.concatenate([qall[chip * 2 + q], ones_ext], axis=1) for q in (0, 1)]

    def score(blocks, chip, j):
        docs = ext[pl.ds(pl.multiple_of(j * DLEN, DLEN), DLEN), :]
        for q in (0, 1):
            sim = lax.dot_general(docs, blocks[q], (((1,), (1,)), ((), ())), preferred_element_type=F32)
            best = jnp.max(sim.reshape(DLEN // 8, 8, TILE), axis=0)
            rs[q, pl.ds(chip * DOCS + j, 1), :] = jnp.max(best, axis=0, keepdims=True)

    def project_step(t, _):
        for n in range(STEP // CHUNK):
            chunk = t * (STEP // CHUNK) + n
            chunk_copy(chunk).wait()

            @pl.when(chunk < NCHUNK - AHEAD)
            def _():
                chunk_copy(chunk + AHEAD).start()

        @pl.when(t == NSTEP - 1)
        def _():
            for k in range(1, SGROUP):
                recv_block(k).wait_recv()
                forward(k).start()

        row = pl.multiple_of(t * STEP, STEP)
        ext[pl.ds(row, STEP), 0:128] = unit(dot(x[pl.ds(row, STEP), :], wv[...])).astype(BF16)
        for n in range(STEP // TILE):
            part = bias[pl.ds((n % 3) * TILE, TILE), :]
            ext[pl.ds(row + n * TILE, TILE), 128:256] = jnp.where(lane == t * 2 + n // 3, part, 0.0).astype(BF16)
        return 0

    pl.semaphore_wait(barrier, NBLK - 1)
    forward(0).start()
    for k in range(1, NCHIP):
        send_block(k).start()
    lax.fori_loop(0, NSTEP, project_step, 0)

    def stages(i, _):
        for n in range(SGROUP):
            recv_forward(i * SGROUP + n).wait_recv()

        @pl.when(i < NCHIP // SGROUP - 1)
        def _():
            for n in range(SGROUP):
                recv_block((i + 1) * SGROUP + n).wait_recv()
                forward((i + 1) * SGROUP + n).start()

        for n in range(SGROUP):
            chip = chip_of(i * SGROUP + n)
            blocks = query_blocks(chip)
            for j in range(DOCS):
                score(blocks, chip, j)
        return 0

    lax.fori_loop(0, NCHIP // SGROUP, stages, 0)

    half = lax.broadcasted_iota(jnp.int32, (DOCS, 128), 1)
    vals = []
    for b in range(NBLK):
        v = rs[b % 2, pl.ds(8 * (b // 2), 8), :]
        vals.append(v[:, :128] + v[:, 128:])
    for width in (64, 32, 16, 8):
        n = len(vals) // 2
        low = (half // width) % 2 == 0
        nxt = []
        for i in range(n):
            keep = jnp.where(low, vals[i], vals[i + n])
            move = jnp.where(low, vals[i + n], vals[i])
            fold = jnp.where(low, pltpu.roll(move, 128 - width, axis=1), pltpu.roll(move, width, axis=1)) if width < 64 else pltpu.roll(move, 64, axis=1)
            nxt.append(keep + fold)
        vals = nxt
    sall[me] = vals[0]

    for k in range(1, NBLK):
        send_scores(k).start()
    for k in range(1, NBLK):
        recv_scores(k).wait_recv()
    out_ref[...] = sall[...]

    for k in range(1, NCHIP):
        send_block(k).wait_send()
    for k in range(NCHIP):
        forward(k).wait_send()
    for k in range(1, NBLK):
        send_scores(k).wait_send()


def loss_kernel(s_ref, t_ref, loss_ref, mean_ref):
    me = lax.axis_index('data2') * 4 + lax.axis_index('data')
    logits = s_ref[...] / t_ref[0]
    top = jnp.max(jnp.max(logits, axis=0), axis=0, keepdims=True)
    total = jnp.sum(jnp.sum(jnp.exp(logits - top[None]), axis=0), axis=0, keepdims=True)
    doc = lax.broadcasted_iota(jnp.int32, (NBLK, DOCS, 128), 0) * DOCS + lax.broadcasted_iota(jnp.int32, (NBLK, DOCS, 128), 1)
    own = doc == lax.broadcasted_iota(jnp.int32, (NBLK, DOCS, 128), 2)
    pos = jnp.sum(jnp.sum(jnp.where(own, logits, 0.0), axis=0), axis=0, keepdims=True)
    loss = top + jnp.log(total) - pos
    mean_ref[...] = jnp.sum(loss, axis=1, keepdims=True) / (NBLK * DOCS)
    loss_ref[...] = pltpu.roll(jnp.broadcast_to(loss, (8, 128)), lax.rem(128 - me * DOCS, 128), axis=1)[0:1, :DOCS]


def solution(mesh):
    def device_fn(q_hidden, d_hidden, w_proj, q_mask, d_mask, temperature):
        hbm = pl.BlockSpec(memory_space=pltpu.HBM)
        vmem = pl.BlockSpec(memory_space=pltpu.VMEM)
        dma = pltpu.SemaphoreType.DMA
        scores = pl.pallas_call(
            kernel,
            out_shape=jax.ShapeDtypeStruct((NBLK, DOCS, 128), F32),
            in_specs=[hbm] * 5,
            out_specs=vmem,
            scratch_shapes=[
                pltpu.VMEM((ROWS, HID), BF16),
                pltpu.VMEM((QROWS, HID), BF16),
                pltpu.VMEM((HID, PROJ), BF16),
                pltpu.VMEM((ROWS, 256), BF16),
                pltpu.VMEM((NBLK, QROWS, PROJ), BF16),
                pltpu.VMEM((QROWS, PROJ), F32),
                pltpu.VMEM((DLEN, 128), F32),
                pltpu.VMEM((2, DOCS * NCHIP, 256), F32),
                pltpu.VMEM((NBLK, DOCS, 128), F32),
                pltpu.VMEM((DOCS, QLEN), jnp.int32),
                pltpu.VMEM((DOCS, DLEN), jnp.int32),
                dma((NCHUNK,)), dma((4,)), dma((NCHIP,)), dma((NCHIP,)), dma((NCHIP,)), dma((NCHIP,)), dma((NBLK,)), dma((NBLK,)),
            ],
            compiler_params=pltpu.CompilerParams(collective_id=0, has_side_effects=True, vmem_limit_bytes=60 * 2**20),
            name='late_interaction',
        )(q_hidden.reshape(QROWS, HID), d_hidden.reshape(ROWS, HID), w_proj, q_mask, d_mask)
        loss, mean = pl.pallas_call(
            loss_kernel,
            out_shape=(jax.ShapeDtypeStruct((1, DOCS), F32), jax.ShapeDtypeStruct((1, 1), F32)),
            in_specs=[vmem, pl.BlockSpec(memory_space=pltpu.SMEM)],
            out_specs=(vmem, vmem),
            name='loss',
        )(scores, temperature.reshape(1))
        return loss.reshape(DOCS), mean.reshape(1)

    return jax.shard_map(
        device_fn,
        mesh=mesh,
        in_specs=(P(ROW_AXES), P(ROW_AXES), P(), P(ROW_AXES), P(ROW_AXES), P()),
        out_specs=(P(ROW_AXES), P('replica')),
        check_vma=False,
    )
```

```python
import jax
import jax.numpy as jnp
from jax import lax
from jax.experimental import pallas as pl
from jax.experimental.pallas import tpu as pltpu
from jax.sharding import PartitionSpec as P

NORM_EPS = 1e-6
ROW_AXES = ('replica', 'data2', 'data')
MESH = pl.DeviceIdType.MESH
F32, BF16 = jnp.float32, jnp.bfloat16
MASKED = -1e30

DOCS, DLEN, QLEN, HID, PROJ = 8, 768, 32, 2048, 128
ROWS = DOCS * DLEN
CHUNK = 768
NCHUNK = ROWS // CHUNK
FIRST = 2
AHEAD = 4
STEP = 768
NSTEP = ROWS // STEP
SGROUP = 2
TILE = 256
QROWS = DOCS * QLEN
NBLK, NCHIP = 16, 8


def kernel(q_hbm, d_hbm, w_hbm, qm_hbm, dm_hbm, out_ref,
           x, qh, wv, ext, qall, qf, bias, rs, sall, qm, dm,
           dsem, isem, bsend, brecv, fsend, frecv, ssend, srecv):
    z, d = lax.axis_index('data2'), lax.axis_index('data')
    y, c = d // 2, d % 2
    me = z * 4 + d

    def peer(k):
        ky, k0, k1 = k % 2, (k // 2) % 2, k // 4
        pz = (z % 2 + k0) % 2 + 2 * ((z // 2 + k1) % 2)
        return pz, ((y + ky) % 2) * 2 + c

    def chip_of(k):
        pz, pd = peer(k)
        return pz * 2 + pd // 2

    def send_block(k):
        pz, pd = peer(k)
        return pltpu.make_async_remote_copy(
            src_ref=qall.at[me], dst_ref=qall.at[me], send_sem=bsend.at[k], recv_sem=brecv.at[k],
            device_id={'data2': pz, 'data': pd}, device_id_type=MESH)

    def recv_block(k):
        pz, pd = peer(k)
        blk = pz * 4 + pd
        return pltpu.make_async_remote_copy(
            src_ref=qall.at[blk], dst_ref=qall.at[blk], send_sem=bsend.at[k], recv_sem=brecv.at[k],
            device_id={'data2': pz, 'data': pd}, device_id_type=MESH)

    def forward(k):
        blk = chip_of(k) * 2 + c
        return pltpu.make_async_remote_copy(
            src_ref=qall.at[blk], dst_ref=qall.at[blk], send_sem=fsend.at[k], recv_sem=frecv.at[k],
            device_id={'data2': z, 'data': y * 2 + 1 - c}, device_id_type=MESH)

    def recv_forward(k):
        blk = chip_of(k) * 2 + 1 - c
        return pltpu.make_async_remote_copy(
            src_ref=qall.at[blk], dst_ref=qall.at[blk], send_sem=fsend.at[k], recv_sem=frecv.at[k],
            device_id={'data2': z, 'data': y * 2 + 1 - c}, device_id_type=MESH)

    def any_peer(k):
        pz, pd = peer(k // 2)
        return pz, (pd // 2) * 2 + (c + k % 2) % 2

    def send_scores(k):
        pz, pd = any_peer(k)
        return pltpu.make_async_remote_copy(
            src_ref=sall.at[me], dst_ref=sall.at[me], send_sem=ssend.at[k], recv_sem=srecv.at[k],
            device_id={'data2': pz, 'data': pd}, device_id_type=MESH)

    def recv_scores(k):
        pz, pd = any_peer(k)
        blk = pz * 4 + pd
        return pltpu.make_async_remote_copy(
            src_ref=sall.at[blk], dst_ref=sall.at[blk], send_sem=ssend.at[k], recv_sem=srecv.at[k],
            device_id={'data2': pz, 'data': pd}, device_id_type=MESH)

    def chunk_copy(t):
        return pltpu.make_async_copy(d_hbm.at[pl.ds(pl.multiple_of(t * CHUNK, CHUNK), CHUNK), :],
                                     x.at[pl.ds(pl.multiple_of(t * CHUNK, CHUNK), CHUNK), :], dsem.at[t])

    copies = [pltpu.make_async_copy(a, b, isem.at[i]) for i, (a, b) in enumerate(
        ((w_hbm, wv), (q_hbm, qh), (qm_hbm, qm), (dm_hbm, dm)))]
    for copy in copies:
        copy.start()
    for t in range(FIRST):
        chunk_copy(t).start()

    barrier = pltpu.get_barrier_semaphore()
    for k in range(1, NBLK):
        pz, pd = any_peer(k)
        pl.semaphore_signal(barrier, inc=1, device_id={'data2': pz, 'data': pd}, device_id_type=MESH)

    def unit(proj):
        return proj * lax.rsqrt(jnp.sum(proj * proj, axis=1, keepdims=True) + NORM_EPS)

    def dot(a, b):
        return lax.dot_general(a, b, (((1,), (0,)), ((), ())), preferred_element_type=F32)

    for i in range(3):
        copies[i].wait()
    for t in range(FIRST, AHEAD):
        chunk_copy(t).start()
    qf[...] = unit(dot(qh[...], wv[...]))
    rows = []
    for t in range(QLEN):
        keep = qm[:, t:t + 1] > 0
        rows.append(jnp.where(keep, qf[pl.ds(t, DOCS, stride=QLEN), :], 0.0))
    qall[me] = jnp.concatenate(rows, axis=0).astype(BF16)

    copies[3].wait()
    pad = jnp.where(dm[...] > 0, 0.0, MASKED).astype(F32)
    pad = jnp.concatenate([pad, jnp.zeros((120, DLEN), F32)], axis=0)
    for i in range(DLEN // 128):
        bias[pl.ds(i * 128, 128), :] = pad[:, i * 128:(i + 1) * 128].T
    lane = lax.broadcasted_iota(jnp.int32, (TILE, 128), 1)

    ones_ext = jnp.where(lane < DOCS, 1.0, 0.0).astype(BF16)

    def query_blocks(chip):
        return [jnp.concatenate([qall[chip * 2 + q], ones_ext], axis=1) for q in (0, 1)]

    def score(blocks, chip, j):
        docs = ext[pl.ds(pl.multiple_of(j * DLEN, DLEN), DLEN), :]
        for q in (0, 1):
            sim = lax.dot_general(docs, blocks[q], (((1,), (1,)), ((), ())), preferred_element_type=F32)
            best = jnp.max(sim.reshape(DLEN // 8, 8, TILE), axis=0)
            rs[q, pl.ds(chip * DOCS + j, 1), :] = jnp.max(best, axis=0, keepdims=True)

    def project_step(t, _):
        for n in range(STEP // CHUNK):
            chunk = t * (STEP // CHUNK) + n
            chunk_copy(chunk).wait()

            @pl.when(chunk < NCHUNK - AHEAD)
            def _():
                chunk_copy(chunk + AHEAD).start()

        @pl.when(t == NSTEP - 1)
        def _():
            for k in range(1, SGROUP):
                recv_block(k).wait_recv()
                forward(k).start()

        row = pl.multiple_of(t * STEP, STEP)
        ext[pl.ds(row, STEP), 0:128] = unit(dot(x[pl.ds(row, STEP), :], wv[...])).astype(BF16)
        for n in range(STEP // TILE):
            part = bias[pl.ds((n % 3) * TILE, TILE), :]
            ext[pl.ds(row + n * TILE, TILE), 128:256] = jnp.where(lane == t * (STEP // DLEN) + n // 3, part, 0.0).astype(BF16)
        return 0

    pl.semaphore_wait(barrier, NBLK - 1)
    forward(0).start()
    for k in range(1, NCHIP):
        send_block(k).start()
    lax.fori_loop(0, NSTEP, project_step, 0)

    def stages(i, _):
        for n in range(SGROUP):
            recv_forward(i * SGROUP + n).wait_recv()

        @pl.when(i < NCHIP // SGROUP - 1)
        def _():
            for n in range(SGROUP):
                recv_block((i + 1) * SGROUP + n).wait_recv()
                forward((i + 1) * SGROUP + n).start()

        for n in range(SGROUP):
            chip = chip_of(i * SGROUP + n)
            blocks = query_blocks(chip)
            for j in range(DOCS):
                score(blocks, chip, j)
        return 0

    lax.fori_loop(0, NCHIP // SGROUP, stages, 0)

    half = lax.broadcasted_iota(jnp.int32, (DOCS, 128), 1)
    vals = []
    for b in range(NBLK):
        v = rs[b % 2, pl.ds(8 * (b // 2), 8), :]
        vals.append(v[:, :128] + v[:, 128:])
    for width in (64, 32, 16, 8):
        n = len(vals) // 2
        low = (half // width) % 2 == 0
        nxt = []
        for i in range(n):
            keep = jnp.where(low, vals[i], vals[i + n])
            move = jnp.where(low, vals[i + n], vals[i])
            fold = jnp.where(low, pltpu.roll(move, 128 - width, axis=1), pltpu.roll(move, width, axis=1)) if width < 64 else pltpu.roll(move, 64, axis=1)
            nxt.append(keep + fold)
        vals = nxt
    sall[me] = vals[0]

    for k in range(1, NBLK):
        send_scores(k).start()
    for k in range(1, NBLK):
        recv_scores(k).wait_recv()
    out_ref[...] = sall[...]

    for k in range(1, NCHIP):
        send_block(k).wait_send()
    for k in range(NCHIP):
        forward(k).wait_send()
    for k in range(1, NBLK):
        send_scores(k).wait_send()


def loss_kernel(s_ref, t_ref, loss_ref, mean_ref):
    me = lax.axis_index('data2') * 4 + lax.axis_index('data')
    logits = s_ref[...] / t_ref[0]
    top = jnp.max(jnp.max(logits, axis=0), axis=0, keepdims=True)
    total = jnp.sum(jnp.sum(jnp.exp(logits - top[None]), axis=0), axis=0, keepdims=True)
    doc = lax.broadcasted_iota(jnp.int32, (NBLK, DOCS, 128), 0) * DOCS + lax.broadcasted_iota(jnp.int32, (NBLK, DOCS, 128), 1)
    own = doc == lax.broadcasted_iota(jnp.int32, (NBLK, DOCS, 128), 2)
    pos = jnp.sum(jnp.sum(jnp.where(own, logits, 0.0), axis=0), axis=0, keepdims=True)
    loss = top + jnp.log(total) - pos
    mean_ref[...] = jnp.sum(loss, axis=1, keepdims=True) / (NBLK * DOCS)
    loss_ref[...] = pltpu.roll(jnp.broadcast_to(loss, (8, 128)), lax.rem(128 - me * DOCS, 128), axis=1)[0:1, :DOCS]


def solution(mesh):
    def device_fn(q_hidden, d_hidden, w_proj, q_mask, d_mask, temperature):
        hbm = pl.BlockSpec(memory_space=pltpu.HBM)
        vmem = pl.BlockSpec(memory_space=pltpu.VMEM)
        dma = pltpu.SemaphoreType.DMA
        scores = pl.pallas_call(
            kernel,
            out_shape=pltpu.VMEM((NBLK, DOCS, 128), F32),
            in_specs=[hbm] * 5,
            out_specs=vmem,
            scratch_shapes=[
                pltpu.VMEM((ROWS, HID), BF16),
                pltpu.VMEM((QROWS, HID), BF16),
                pltpu.VMEM((HID, PROJ), BF16),
                pltpu.VMEM((ROWS, 256), BF16),
                pltpu.VMEM((NBLK, QROWS, PROJ), BF16),
                pltpu.VMEM((QROWS, PROJ), F32),
                pltpu.VMEM((DLEN, 128), F32),
                pltpu.VMEM((2, DOCS * NCHIP, 256), F32),
                pltpu.VMEM((NBLK, DOCS, 128), F32),
                pltpu.VMEM((DOCS, QLEN), jnp.int32),
                pltpu.VMEM((DOCS, DLEN), jnp.int32),
                dma((NCHUNK,)), dma((4,)), dma((NCHIP,)), dma((NCHIP,)), dma((NCHIP,)), dma((NCHIP,)), dma((NBLK,)), dma((NBLK,)),
            ],
            compiler_params=pltpu.CompilerParams(collective_id=0, has_side_effects=True, vmem_limit_bytes=60 * 2**20),
            name='late_interaction',
        )(q_hidden.reshape(QROWS, HID), d_hidden.reshape(ROWS, HID), w_proj, q_mask, d_mask)
        loss, mean = pl.pallas_call(
            loss_kernel,
            out_shape=(jax.ShapeDtypeStruct((1, DOCS), F32), jax.ShapeDtypeStruct((1, 1), F32)),
            in_specs=[vmem, pl.BlockSpec(memory_space=pltpu.SMEM)],
            out_specs=(vmem, vmem),
            name='loss',
        )(pltpu.with_memory_space_constraint(scores, pltpu.VMEM), temperature.reshape(1))
        return loss.reshape(DOCS), mean.reshape(1)

    return jax.shard_map(
        device_fn,
        mesh=mesh,
        in_specs=(P(ROW_AXES), P(ROW_AXES), P(), P(ROW_AXES), P(ROW_AXES), P()),
        out_specs=(P(ROW_AXES), P('replica')),
        check_vma=False,
    )
```

```python
import jax
import jax.numpy as jnp
from jax import lax
from jax.experimental import pallas as pl
from jax.experimental.pallas import tpu as pltpu
from jax.sharding import PartitionSpec as P

NORM_EPS = 1e-6
ROW_AXES = ('replica', 'data2', 'data')
MESH = pl.DeviceIdType.MESH
F32, BF16 = jnp.float32, jnp.bfloat16
MASKED = -1e30

DOCS, DLEN, QLEN, HID, PROJ = 8, 768, 32, 2048, 128
ROWS = DOCS * DLEN
CHUNK = 768
NCHUNK = ROWS // CHUNK
FIRST = 2
AHEAD = 4
STEP = 768
NSTEP = ROWS // STEP
SGROUP = 2
TILE = 256
QROWS = DOCS * QLEN
NBLK, NCHIP = 16, 8


def kernel(q_hbm, d_hbm, w_hbm, qm_hbm, dm_hbm, out_ref,
           x, qh, wv, ext, qall, qf, bias, rs, sall, qm, dm,
           dsem, isem, bsend, brecv, fsend, frecv, ssend, srecv):
    z, d = lax.axis_index('data2'), lax.axis_index('data')
    y, c = d // 2, d % 2
    me = z * 4 + d

    def peer(k):
        ky, k0, k1 = k % 2, (k // 2) % 2, k // 4
        pz = (z % 2 + k0) % 2 + 2 * ((z // 2 + k1) % 2)
        return pz, ((y + ky) % 2) * 2 + c

    def chip_of(k):
        pz, pd = peer(k)
        return pz * 2 + pd // 2

    def send_block(k):
        pz, pd = peer(k)
        return pltpu.make_async_remote_copy(
            src_ref=qall.at[me], dst_ref=qall.at[me], send_sem=bsend.at[k], recv_sem=brecv.at[k],
            device_id={'data2': pz, 'data': pd}, device_id_type=MESH)

    def recv_block(k):
        pz, pd = peer(k)
        blk = pz * 4 + pd
        return pltpu.make_async_remote_copy(
            src_ref=qall.at[blk], dst_ref=qall.at[blk], send_sem=bsend.at[k], recv_sem=brecv.at[k],
            device_id={'data2': pz, 'data': pd}, device_id_type=MESH)

    def forward(k):
        blk = chip_of(k) * 2 + c
        return pltpu.make_async_remote_copy(
            src_ref=qall.at[blk], dst_ref=qall.at[blk], send_sem=fsend.at[k], recv_sem=frecv.at[k],
            device_id={'data2': z, 'data': y * 2 + 1 - c}, device_id_type=MESH)

    def recv_forward(k):
        blk = chip_of(k) * 2 + 1 - c
        return pltpu.make_async_remote_copy(
            src_ref=qall.at[blk], dst_ref=qall.at[blk], send_sem=fsend.at[k], recv_sem=frecv.at[k],
            device_id={'data2': z, 'data': y * 2 + 1 - c}, device_id_type=MESH)

    def any_peer(k):
        pz, pd = peer(k // 2)
        return pz, (pd // 2) * 2 + (c + k % 2) % 2

    def send_scores(k):
        pz, pd = any_peer(k)
        return pltpu.make_async_remote_copy(
            src_ref=sall.at[me], dst_ref=sall.at[me], send_sem=ssend.at[k], recv_sem=srecv.at[k],
            device_id={'data2': pz, 'data': pd}, device_id_type=MESH)

    def recv_scores(k):
        pz, pd = any_peer(k)
        blk = pz * 4 + pd
        return pltpu.make_async_remote_copy(
            src_ref=sall.at[blk], dst_ref=sall.at[blk], send_sem=ssend.at[k], recv_sem=srecv.at[k],
            device_id={'data2': pz, 'data': pd}, device_id_type=MESH)

    def chunk_copy(t):
        return pltpu.make_async_copy(d_hbm.at[pl.ds(pl.multiple_of(t * CHUNK, CHUNK), CHUNK), :],
                                     x.at[pl.ds(pl.multiple_of(t * CHUNK, CHUNK), CHUNK), :], dsem.at[t])

    copies = [pltpu.make_async_copy(a, b, isem.at[i]) for i, (a, b) in enumerate(
        ((w_hbm, wv), (q_hbm, qh), (qm_hbm, qm), (dm_hbm, dm)))]
    for copy in copies:
        copy.start()
    for t in range(FIRST):
        chunk_copy(t).start()

    barrier = pltpu.get_barrier_semaphore()
    for k in range(NBLK - 1, 0, -1):
        pz, pd = any_peer(k)
        pl.semaphore_signal(barrier, inc=1, device_id={'data2': pz, 'data': pd}, device_id_type=MESH)

    def unit(proj):
        return proj * lax.rsqrt(jnp.sum(proj * proj, axis=1, keepdims=True) + NORM_EPS)

    def dot(a, b):
        return lax.dot_general(a, b, (((1,), (0,)), ((), ())), preferred_element_type=F32)

    for i in range(3):
        copies[i].wait()
    for t in range(FIRST, AHEAD):
        chunk_copy(t).start()
    qf[...] = unit(dot(qh[...], wv[...]))
    rows = []
    for t in range(QLEN):
        keep = qm[:, t:t + 1] > 0
        rows.append(jnp.where(keep, qf[pl.ds(t, DOCS, stride=QLEN), :], 0.0))
    qall[me] = jnp.concatenate(rows, axis=0).astype(BF16)

    copies[3].wait()
    pad = jnp.where(dm[...] > 0, 0.0, MASKED).astype(F32)
    pad = jnp.concatenate([pad, jnp.zeros((120, DLEN), F32)], axis=0)
    for i in range(DLEN // 128):
        bias[pl.ds(i * 128, 128), :] = pad[:, i * 128:(i + 1) * 128].T
    lane = lax.broadcasted_iota(jnp.int32, (TILE, 128), 1)

    ones_ext = jnp.where(lane < DOCS, 1.0, 0.0).astype(BF16)

    def query_blocks(chip):
        return [jnp.concatenate([qall[chip * 2 + q], ones_ext], axis=1) for q in (0, 1)]

    def score(blocks, chip, j):
        docs = ext[pl.ds(pl.multiple_of(j * DLEN, DLEN), DLEN), :]
        for q in (0, 1):
            sim = lax.dot_general(docs, blocks[q], (((1,), (1,)), ((), ())), preferred_element_type=F32)
            best = jnp.max(sim.reshape(DLEN // 8, 8, TILE), axis=0)
            rs[q, pl.ds(chip * DOCS + j, 1), :] = jnp.max(best, axis=0, keepdims=True)

    def project_step(t, _):
        for n in range(STEP // CHUNK):
            chunk = t * (STEP // CHUNK) + n
            chunk_copy(chunk).wait()

            @pl.when(chunk < NCHUNK - AHEAD)
            def _():
                chunk_copy(chunk + AHEAD).start()

        @pl.when(t == NSTEP - 1)
        def _():
            for k in range(1, SGROUP):
                recv_block(k).wait_recv()
                forward(k).start()

        row = pl.multiple_of(t * STEP, STEP)
        ext[pl.ds(row, STEP), 0:128] = unit(dot(x[pl.ds(row, STEP), :], wv[...])).astype(BF16)
        for n in range(STEP // TILE):
            part = bias[pl.ds((n % 3) * TILE, TILE), :]
            ext[pl.ds(row + n * TILE, TILE), 128:256] = jnp.where(lane == t * (STEP // DLEN) + n // 3, part, 0.0).astype(BF16)
        return 0

    pl.semaphore_wait(barrier, NBLK - 1)
    forward(0).start()
    for k in range(1, NCHIP):
        send_block(k).start()
    lax.fori_loop(0, NSTEP, project_step, 0)

    def stages(i, _):
        for n in range(SGROUP):
            recv_forward(i * SGROUP + n).wait_recv()

        @pl.when(i < NCHIP // SGROUP - 1)
        def _():
            for n in range(SGROUP):
                recv_block((i + 1) * SGROUP + n).wait_recv()
                forward((i + 1) * SGROUP + n).start()

        for n in range(SGROUP):
            chip = chip_of(i * SGROUP + n)
            blocks = query_blocks(chip)
            for j in range(DOCS):
                score(blocks, chip, j)
        return 0

    lax.fori_loop(0, NCHIP // SGROUP, stages, 0)

    half = lax.broadcasted_iota(jnp.int32, (DOCS, 128), 1)
    vals = []
    for b in range(NBLK):
        v = rs[b % 2, pl.ds(8 * (b // 2), 8), :]
        vals.append(v[:, :128] + v[:, 128:])
    for width in (64, 32, 16, 8):
        n = len(vals) // 2
        low = (half // width) % 2 == 0
        nxt = []
        for i in range(n):
            keep = jnp.where(low, vals[i], vals[i + n])
            move = jnp.where(low, vals[i + n], vals[i])
            fold = jnp.where(low, pltpu.roll(move, 128 - width, axis=1), pltpu.roll(move, width, axis=1)) if width < 64 else pltpu.roll(move, 64, axis=1)
            nxt.append(keep + fold)
        vals = nxt
    sall[me] = vals[0]

    for k in range(NBLK - 1, 0, -1):
        send_scores(k).start()
    for k in range(1, NBLK):
        recv_scores(k).wait_recv()
    out_ref[...] = sall[...]

    for k in range(1, NCHIP):
        send_block(k).wait_send()
    for k in range(NCHIP):
        forward(k).wait_send()
    for k in range(1, NBLK):
        send_scores(k).wait_send()


def loss_kernel(s_ref, t_ref, loss_ref, mean_ref):
    me = lax.axis_index('data2') * 4 + lax.axis_index('data')
    logits = s_ref[...] / t_ref[0]
    top = jnp.max(jnp.max(logits, axis=0), axis=0, keepdims=True)
    total = jnp.sum(jnp.sum(jnp.exp(logits - top[None]), axis=0), axis=0, keepdims=True)
    doc = lax.broadcasted_iota(jnp.int32, (NBLK, DOCS, 128), 0) * DOCS + lax.broadcasted_iota(jnp.int32, (NBLK, DOCS, 128), 1)
    own = doc == lax.broadcasted_iota(jnp.int32, (NBLK, DOCS, 128), 2)
    pos = jnp.sum(jnp.sum(jnp.where(own, logits, 0.0), axis=0), axis=0, keepdims=True)
    loss = top + jnp.log(total) - pos
    mean_ref[...] = jnp.sum(loss, axis=1, keepdims=True) / (NBLK * DOCS)
    loss_ref[...] = pltpu.roll(jnp.broadcast_to(loss, (8, 128)), lax.rem(128 - me * DOCS, 128), axis=1)[0:1, :DOCS]


def solution(mesh):
    def device_fn(q_hidden, d_hidden, w_proj, q_mask, d_mask, temperature):
        hbm = pl.BlockSpec(memory_space=pltpu.HBM)
        vmem = pl.BlockSpec(memory_space=pltpu.VMEM)
        dma = pltpu.SemaphoreType.DMA
        scores = pl.pallas_call(
            kernel,
            out_shape=pltpu.VMEM((NBLK, DOCS, 128), F32),
            in_specs=[hbm] * 5,
            out_specs=vmem,
            scratch_shapes=[
                pltpu.VMEM((ROWS, HID), BF16),
                pltpu.VMEM((QROWS, HID), BF16),
                pltpu.VMEM((HID, PROJ), BF16),
                pltpu.VMEM((ROWS, 256), BF16),
                pltpu.VMEM((NBLK, QROWS, PROJ), BF16),
                pltpu.VMEM((QROWS, PROJ), F32),
                pltpu.VMEM((DLEN, 128), F32),
                pltpu.VMEM((2, DOCS * NCHIP, 256), F32),
                pltpu.VMEM((NBLK, DOCS, 128), F32),
                pltpu.VMEM((DOCS, QLEN), jnp.int32),
                pltpu.VMEM((DOCS, DLEN), jnp.int32),
                dma((NCHUNK,)), dma((4,)), dma((NCHIP,)), dma((NCHIP,)), dma((NCHIP,)), dma((NCHIP,)), dma((NBLK,)), dma((NBLK,)),
            ],
            compiler_params=pltpu.CompilerParams(collective_id=0, has_side_effects=True, vmem_limit_bytes=60 * 2**20),
            name='late_interaction',
        )(q_hidden.reshape(QROWS, HID), d_hidden.reshape(ROWS, HID), w_proj, q_mask, d_mask)
        loss, mean = pl.pallas_call(
            loss_kernel,
            out_shape=(jax.ShapeDtypeStruct((1, DOCS), F32), jax.ShapeDtypeStruct((1, 1), F32)),
            in_specs=[vmem, pl.BlockSpec(memory_space=pltpu.SMEM)],
            out_specs=(vmem, vmem),
            name='loss',
        )(pltpu.with_memory_space_constraint(scores, pltpu.VMEM), temperature.reshape(1))
        return loss.reshape(DOCS), mean.reshape(1)

    return jax.shard_map(
        device_fn,
        mesh=mesh,
        in_specs=(P(ROW_AXES), P(ROW_AXES), P(), P(ROW_AXES), P(ROW_AXES), P()),
        out_specs=(P(ROW_AXES), P('replica')),
        check_vma=False,
    )
```

```python
import jax
import jax.numpy as jnp
from jax import lax
from jax.experimental import pallas as pl
from jax.experimental.pallas import tpu as pltpu
from jax.sharding import PartitionSpec as P

NORM_EPS = 1e-6
ROW_AXES = ('replica', 'data2', 'data')
MESH = pl.DeviceIdType.MESH
F32, BF16 = jnp.float32, jnp.bfloat16
MASKED = -1e30

DOCS, DLEN, QLEN, HID, PROJ = 8, 768, 32, 2048, 128
ROWS = DOCS * DLEN
CHUNK = 768
NCHUNK = ROWS // CHUNK
FIRST = 2
AHEAD = 4
STEP = 768
NSTEP = ROWS // STEP
SGROUP = 2
TILE = 256
QROWS = DOCS * QLEN
NBLK, NCHIP = 16, 8


def kernel(q_hbm, d_hbm, w_hbm, qm_hbm, dm_hbm, out_ref,
           x, qh, wv, ext, qall, qf, bias, rs, sall, qm, dm,
           dsem, isem, bsend, brecv, fsend, frecv, ssend, srecv):
    z, d = lax.axis_index('data2'), lax.axis_index('data')
    y, c = d // 2, d % 2
    me = z * 4 + d

    def peer(k):
        ky, k0, k1 = k % 2, (k // 2) % 2, k // 4
        pz = (z % 2 + k0) % 2 + 2 * ((z // 2 + k1) % 2)
        return pz, ((y + ky) % 2) * 2 + c

    def chip_of(k):
        pz, pd = peer(k)
        return pz * 2 + pd // 2

    def send_block(k):
        pz, pd = peer(k)
        return pltpu.make_async_remote_copy(
            src_ref=qall.at[me], dst_ref=qall.at[me], send_sem=bsend.at[k], recv_sem=brecv.at[k],
            device_id={'data2': pz, 'data': pd}, device_id_type=MESH)

    def recv_block(k):
        pz, pd = peer(k)
        blk = pz * 4 + pd
        return pltpu.make_async_remote_copy(
            src_ref=qall.at[blk], dst_ref=qall.at[blk], send_sem=bsend.at[k], recv_sem=brecv.at[k],
            device_id={'data2': pz, 'data': pd}, device_id_type=MESH)

    def forward(k):
        blk = chip_of(k) * 2 + c
        return pltpu.make_async_remote_copy(
            src_ref=qall.at[blk], dst_ref=qall.at[blk], send_sem=fsend.at[k], recv_sem=frecv.at[k],
            device_id={'data2': z, 'data': y * 2 + 1 - c}, device_id_type=MESH)

    def recv_forward(k):
        blk = chip_of(k) * 2 + 1 - c
        return pltpu.make_async_remote_copy(
            src_ref=qall.at[blk], dst_ref=qall.at[blk], send_sem=fsend.at[k], recv_sem=frecv.at[k],
            device_id={'data2': z, 'data': y * 2 + 1 - c}, device_id_type=MESH)

    def any_peer(k):
        pz, pd = peer(k // 2)
        return pz, (pd // 2) * 2 + (c + k % 2) % 2

    def send_scores(k):
        pz, pd = any_peer(k)
        return pltpu.make_async_remote_copy(
            src_ref=sall.at[me], dst_ref=sall.at[me], send_sem=ssend.at[k], recv_sem=srecv.at[k],
            device_id={'data2': pz, 'data': pd}, device_id_type=MESH)

    def recv_scores(k):
        pz, pd = any_peer(k)
        blk = pz * 4 + pd
        return pltpu.make_async_remote_copy(
            src_ref=sall.at[blk], dst_ref=sall.at[blk], send_sem=ssend.at[k], recv_sem=srecv.at[k],
            device_id={'data2': pz, 'data': pd}, device_id_type=MESH)

    def chunk_copy(t):
        return pltpu.make_async_copy(d_hbm.at[pl.ds(pl.multiple_of(t * CHUNK, CHUNK), CHUNK), :],
                                     x.at[pl.ds(pl.multiple_of(t * CHUNK, CHUNK), CHUNK), :], dsem.at[t])

    copies = [pltpu.make_async_copy(a, b, isem.at[i]) for i, (a, b) in enumerate(
        ((w_hbm, wv), (q_hbm, qh), (qm_hbm, qm), (dm_hbm, dm)))]
    for copy in copies:
        copy.start()
    for t in range(FIRST):
        chunk_copy(t).start()

    barrier = pltpu.get_barrier_semaphore()
    for k in range(NBLK - 1, 0, -1):
        pz, pd = any_peer(k)
        pl.semaphore_signal(barrier, inc=1, device_id={'data2': pz, 'data': pd}, device_id_type=MESH)

    def unit(proj):
        return proj * lax.rsqrt(jnp.sum(proj * proj, axis=1, keepdims=True) + NORM_EPS)

    def dot(a, b):
        return lax.dot_general(a, b, (((1,), (0,)), ((), ())), preferred_element_type=F32)

    for i in range(3):
        copies[i].wait()
    for t in range(FIRST, AHEAD):
        chunk_copy(t).start()
    qf[...] = unit(dot(qh[...], wv[...]))
    rows = []
    for t in range(QLEN):
        keep = qm[:, t:t + 1] > 0
        rows.append(jnp.where(keep, qf[pl.ds(t, DOCS, stride=QLEN), :], 0.0))
    qall[me] = jnp.concatenate(rows, axis=0).astype(BF16)

    copies[3].wait()
    pad = jnp.where(dm[...] > 0, 0.0, MASKED).astype(F32)
    pad = jnp.concatenate([pad, jnp.zeros((120, DLEN), F32)], axis=0)
    for i in range(DLEN // 128):
        bias[pl.ds(i * 128, 128), :] = pad[:, i * 128:(i + 1) * 128].T
    lane = lax.broadcasted_iota(jnp.int32, (TILE, 128), 1)

    ones_ext = jnp.where(lane < DOCS, 1.0, 0.0).astype(BF16)

    def query_blocks(chip):
        return [jnp.concatenate([qall[chip * 2 + q], ones_ext], axis=1) for q in (0, 1)]

    def score(blocks, chip, j):
        docs = ext[pl.ds(pl.multiple_of(j * DLEN, DLEN), DLEN), :]
        for q in (0, 1):
            sim = lax.dot_general(docs, blocks[q], (((1,), (1,)), ((), ())), preferred_element_type=F32)
            best = jnp.max(sim.reshape(DLEN // 8, 8, TILE), axis=0)
            rs[q, pl.ds(chip * DOCS + j, 1), :] = jnp.max(best, axis=0, keepdims=True)

    def project_step(t, _):
        for n in range(STEP // CHUNK):
            chunk = t * (STEP // CHUNK) + n
            chunk_copy(chunk).wait()

            @pl.when(chunk < NCHUNK - AHEAD)
            def _():
                chunk_copy(chunk + AHEAD).start()

        @pl.when(t == NSTEP - 1)
        def _():
            for k in range(1, SGROUP):
                recv_block(k).wait_recv()
                forward(k).start()

        row = pl.multiple_of(t * STEP, STEP)
        ext[pl.ds(row, STEP), 0:128] = unit(dot(x[pl.ds(row, STEP), :], wv[...])).astype(BF16)
        for n in range(STEP // TILE):
            part = bias[pl.ds((n % 3) * TILE, TILE), :]
            ext[pl.ds(row + n * TILE, TILE), 128:256] = jnp.where(lane == t * (STEP // DLEN) + n // 3, part, 0.0).astype(BF16)
        return 0

    pl.semaphore_wait(barrier, NBLK - 1)
    forward(0).start()
    for k in range(1, NCHIP):
        send_block(k).start()
    lax.fori_loop(0, NSTEP, project_step, 0)

    def stages(i, _):
        for n in range(SGROUP):
            recv_forward(i * SGROUP + n).wait_recv()

        @pl.when(i < NCHIP // SGROUP - 1)
        def _():
            for n in range(SGROUP):
                recv_block((i + 1) * SGROUP + n).wait_recv()
                forward((i + 1) * SGROUP + n).start()

        for n in range(SGROUP):
            chip = chip_of(i * SGROUP + n)
            blocks = query_blocks(chip)
            for j in range(DOCS):
                score(blocks, chip, j)
        return 0

    lax.fori_loop(0, NCHIP // SGROUP, stages, 0)

    half = lax.broadcasted_iota(jnp.int32, (DOCS, 128), 1)
    vals = []
    for b in range(NBLK):
        v = rs[b % 2, pl.ds(8 * (b // 2), 8), :]
        vals.append(v[:, :128] + v[:, 128:])
    for width in (64, 32, 16, 8):
        n = len(vals) // 2
        low = (half // width) % 2 == 0
        nxt = []
        for i in range(n):
            keep = jnp.where(low, vals[i], vals[i + n])
            move = jnp.where(low, vals[i + n], vals[i])
            fold = jnp.where(low, pltpu.roll(move, 128 - width, axis=1), pltpu.roll(move, width, axis=1)) if width < 64 else pltpu.roll(move, 64, axis=1)
            nxt.append(keep + fold)
        vals = nxt
    sall[me] = vals[0]

    for k in range(NBLK - 1, 0, -1):
        send_scores(k).start()
    for k in range(1, NCHIP):
        send_block(k).wait_send()
    for k in range(NCHIP):
        forward(k).wait_send()
    for k in range(1, NBLK):
        send_scores(k).wait_send()
    for k in range(1, NBLK):
        recv_scores(k).wait_recv()
    out_ref[...] = sall[...]


def loss_kernel(s_ref, t_ref, loss_ref, mean_ref):
    me = lax.axis_index('data2') * 4 + lax.axis_index('data')
    logits = s_ref[...] / t_ref[0]
    top = jnp.max(jnp.max(logits, axis=0), axis=0, keepdims=True)
    total = jnp.sum(jnp.sum(jnp.exp(logits - top[None]), axis=0), axis=0, keepdims=True)
    doc = lax.broadcasted_iota(jnp.int32, (NBLK, DOCS, 128), 0) * DOCS + lax.broadcasted_iota(jnp.int32, (NBLK, DOCS, 128), 1)
    own = doc == lax.broadcasted_iota(jnp.int32, (NBLK, DOCS, 128), 2)
    pos = jnp.sum(jnp.sum(jnp.where(own, logits, 0.0), axis=0), axis=0, keepdims=True)
    loss = top + jnp.log(total) - pos
    mean_ref[...] = jnp.sum(loss, axis=1, keepdims=True) / (NBLK * DOCS)
    loss_ref[...] = pltpu.roll(jnp.broadcast_to(loss, (8, 128)), lax.rem(128 - me * DOCS, 128), axis=1)[0:1, :DOCS]


def solution(mesh):
    def device_fn(q_hidden, d_hidden, w_proj, q_mask, d_mask, temperature):
        hbm = pl.BlockSpec(memory_space=pltpu.HBM)
        vmem = pl.BlockSpec(memory_space=pltpu.VMEM)
        dma = pltpu.SemaphoreType.DMA
        scores = pl.pallas_call(
            kernel,
            out_shape=pltpu.VMEM((NBLK, DOCS, 128), F32),
            in_specs=[hbm] * 5,
            out_specs=vmem,
            scratch_shapes=[
                pltpu.VMEM((ROWS, HID), BF16),
                pltpu.VMEM((QROWS, HID), BF16),
                pltpu.VMEM((HID, PROJ), BF16),
                pltpu.VMEM((ROWS, 256), BF16),
                pltpu.VMEM((NBLK, QROWS, PROJ), BF16),
                pltpu.VMEM((QROWS, PROJ), F32),
                pltpu.VMEM((DLEN, 128), F32),
                pltpu.VMEM((2, DOCS * NCHIP, 256), F32),
                pltpu.VMEM((NBLK, DOCS, 128), F32),
                pltpu.VMEM((DOCS, QLEN), jnp.int32),
                pltpu.VMEM((DOCS, DLEN), jnp.int32),
                dma((NCHUNK,)), dma((4,)), dma((NCHIP,)), dma((NCHIP,)), dma((NCHIP,)), dma((NCHIP,)), dma((NBLK,)), dma((NBLK,)),
            ],
            compiler_params=pltpu.CompilerParams(collective_id=0, has_side_effects=True, vmem_limit_bytes=60 * 2**20),
            name='late_interaction',
        )(q_hidden.reshape(QROWS, HID), d_hidden.reshape(ROWS, HID), w_proj, q_mask, d_mask)
        loss, mean = pl.pallas_call(
            loss_kernel,
            out_shape=(jax.ShapeDtypeStruct((1, DOCS), F32), jax.ShapeDtypeStruct((1, 1), F32)),
            in_specs=[vmem, pl.BlockSpec(memory_space=pltpu.SMEM)],
            out_specs=(vmem, vmem),
            name='loss',
        )(pltpu.with_memory_space_constraint(scores, pltpu.VMEM), temperature.reshape(1))
        return loss.reshape(DOCS), mean.reshape(1)

    return jax.shard_map(
        device_fn,
        mesh=mesh,
        in_specs=(P(ROW_AXES), P(ROW_AXES), P(), P(ROW_AXES), P(ROW_AXES), P()),
        out_specs=(P(ROW_AXES), P('replica')),
        check_vma=False,
    )
```
